32 devices in a mesh: batch: 2 (over y), space: 16 (over z, x, core).
Axes of the slice: x: 2, y: 2, z: 4, core: 2. Of those that a mesh axis runs over, the one named last changes fastest.
Arguments:
- features: bfloat16 [2, 80, 64, 512], P('batch', 'space'), may hold values from -6 to 6
- cotangent: bfloat16 [2, 80, 64, 512], P('batch', 'space'), may hold values from -6 to 6
- brick_count: int32 [2, 16], P('batch', 'space'), may hold values from 1 to 5, as said below
- destination: int32 [2, 80], P('batch', 'space'), may hold values from -1 to 31, as said below
- neighbours: int32 [2, 26, 80], P('batch', None, 'space'), may hold values from -1 to 4, as said below
- kernel_one: bfloat16 [64, 1728], replicated, may hold values from -0.15625 to 0.15625
- kernel_two: bfloat16 [64, 1728], replicated, may hold values from -0.15625 to 0.15625
Outputs:
- block_output: bfloat16 [2, 32, 64, 512], P('batch', 'space')
- grad_features: bfloat16 [2, 80, 64, 512], P('batch', 'space')
- grad_kernel_one: float32 [64, 1728], replicated
- grad_kernel_two: float32 [64, 1728], replicated
The draws below stay inside these ranges and needn't reach their ends.
Inputs may be any that keep to these rules, and one draw needn't show every extreme that they name: `brick_count`: A volume holds at most 2 times the devices of space active bricks; some device holds exactly 5. `destination`: -1 exactly on inactive slots. A device's first min(count, 2) bricks go to its own work slots 0, 1, ... in order; its brick in slot 2 + k (k = 0, 1, 2) goes to a work slot of device (s + 1 + k) mod 16; every work slot receives at most one brick, every device receives at most one brick, and a receiving device's own bricks fill its slots below the received one. In every volume some device receives a brick in its work slot 1. `neighbours`: entries of inactive slots are -1; an entry is never the slot of an inactive brick. Bricks sit on a grid of 3 x 3 positions per device, and the offset along the first cell axis is the offset in the device index.
All inputs are finite; a program needn't handle non-finite values.
Results may differ from the reference program's by a relative error of at most 0.0041.
Values may be sent and summed in bfloat16 or wider, within the bound.
No kernel may reach another device: no remote copies, remote signals or barrier semaphores. Data moves between devices by JAX's collectives and lax.ppermute only.
A program may use at most 128 MiB of HBM per device.

```python
import math
from functools import partial
import jax
import jax.numpy as jnp
from jax import lax

C = 64
EDGE = 8
WORK_CAP = 2
HOME_CAP = 5
SIDE = 3
CELLS = 512
GROUPS = 2
SLOTS = 80
N_SPACE = 16


def volume_tables(volume_key):
    devices = N_SPACE
    key_list = jax.random.split(volume_key, 4)
    device_ids = jnp.arange(devices, dtype=jnp.int32)
    slot_ids = jnp.arange(HOME_CAP, dtype=jnp.int32)
    rotation = jax.random.randint(key_list[0], (), 0, devices, dtype=jnp.int32)
    order = ((device_ids + rotation) % devices).astype(jnp.int32)
    rank = ((device_ids - rotation) % devices).astype(jnp.int32)
    leaders = jnp.arange(devices // 4, dtype=jnp.int32)
    extra = jax.random.randint(key_list[1], (devices // 4,), 1, 4, dtype=jnp.int32)
    extra = jnp.where(leaders == 0, 3, extra)
    light = jax.random.randint(key_list[2], (devices,), 1, WORK_CAP, dtype=jnp.int32)
    light = jnp.where(rank == 1, WORK_CAP - 1, light)
    member = rank % 4
    team = rank // 4
    counts = jnp.where(member == 0, WORK_CAP + extra[team], light).astype(jnp.int32)
    kept = slot_ids[None, :] < jnp.minimum(counts, WORK_CAP)[:, None]
    surplus = (member == 0)[:, None] & (slot_ids[None, :] >= WORK_CAP) & (slot_ids[None, :] < counts[:, None])
    partner = order[jnp.clip(team[:, None] * 4 + 1 + slot_ids[None, :] - WORK_CAP, 0, devices - 1)]
    moved = partner * WORK_CAP + counts[partner]
    dests = jnp.where(kept, device_ids[:, None] * WORK_CAP + slot_ids[None, :], jnp.where(surplus, moved, -1))

    def one_place(device_number):
        return jax.random.permutation(jax.random.fold_in(key_list[3], device_number), SIDE * SIDE).astype(jnp.int32)
    places = jax.vmap(one_place)(device_ids)
    lookup = jnp.argsort(places, axis=1).astype(jnp.int32)
    spots = places[:, :HOME_CAP]
    entries = []
    for along_first in (-1, 0, 1):
        for along_second in (-1, 0, 1):
            for along_third in (-1, 0, 1):
                if (along_first, along_second, along_third) == (0, 0, 0):
                    continue
                other = device_ids[:, None] + along_first
                row_pos = spots // SIDE + along_second
                col_pos = spots % SIDE + along_third
                inside = (other >= 0) & (other < devices) & (row_pos >= 0) & (row_pos < SIDE) & (col_pos >= 0) & (col_pos < SIDE)
                other_clip = jnp.clip(other, 0, devices - 1)
                spot_clip = jnp.clip(row_pos, 0, SIDE - 1) * SIDE + jnp.clip(col_pos, 0, SIDE - 1)
                found = lookup[other_clip, spot_clip]
                live = inside & (found < counts[other_clip]) & (slot_ids[None, :] < counts[:, None])
                entries.append(jnp.where(live, found, -1))
    table = jnp.stack(entries).reshape(26, devices * HOME_CAP)
    return (counts, dests.reshape(-1).astype(jnp.int32), table.astype(jnp.int32))


def layout_tables(key):
    base = jax.random.fold_in(key, 17)
    volume_keys = jax.vmap(jax.random.fold_in, in_axes=(None, 0))(base, jnp.arange(GROUPS))
    return jax.vmap(volume_tables)(volume_keys)


def draw_brick_count(key, part):
    return layout_tables(key)[0].astype(jnp.int32)


def draw_destination(key, part):
    return layout_tables(key)[1].astype(jnp.int32)


def draw_neighbours(key, part):
    return layout_tables(key)[2].astype(jnp.int32)


def shard_levels(key, extent, cuts, smallest, high):
    loudness, own = 1.0, jax.random.fold_in(key, 6)
    for axis_at, blocks in cuts:
        heights = jnp.exp(jax.random.uniform(jax.random.fold_in(own, axis_at), (blocks,), jnp.float32, smallest / len(cuts), high / len(cuts)))
        loudness = loudness * jnp.repeat(heights, extent[axis_at] // blocks).reshape([-1 if axis == axis_at else 1 for axis in range(len(extent))])
    return loudness


def normal_values(own_key, dims, scale, limit, shards=(), kind=jnp.bfloat16):
    drawn = scale * jax.random.normal(own_key, dims, jnp.float32)
    if shards:
        drawn = drawn * shard_levels(own_key, dims, shards, -0.22, 0.18)
    return jnp.clip(drawn, -limit, limit).astype(kind)


def setup_inputs(seed: int = 0) -> dict:
    keys = jax.random.split(jax.random.key(seed), 8)
    features = normal_values(keys[0], (GROUPS, SLOTS, C, CELLS), 1.0, 6.0, ((0, 2), (1, 16)))
    cotangent = normal_values(keys[1], (GROUPS, SLOTS, C, CELLS), 1.0, 6.0, ((0, 2), (1, 16)))
    brick_count = draw_brick_count(jax.random.fold_in(keys[7], 71), 0)
    destination = draw_destination(jax.random.fold_in(keys[7], 71), 0)
    neighbours = draw_neighbours(jax.random.fold_in(keys[7], 71), 0)
    kernel_one = normal_values(keys[5], (C, 27 * C), (27 * C) ** -0.5, 0.15625)
    kernel_two = normal_values(keys[6], (C, 27 * C), (27 * C) ** -0.5, 0.15625)
    return {"features": features, "cotangent": cotangent, "brick_count": brick_count, "destination": destination, "neighbours": neighbours, "kernel_one": kernel_one, "kernel_two": kernel_two}


def cut_side(region, axis_number, offset, margin_width):
    if offset < 0:
        return lax.slice_in_dim(region, EDGE - margin_width, EDGE, axis=axis_number)
    if offset > 0:
        return lax.slice_in_dim(region, 0, margin_width, axis=axis_number)
    return region

def pick_rows(source, slot_index):
    present = slot_index >= 0
    chosen = jnp.take(source, jnp.maximum(slot_index, 0).astype(jnp.int32), axis=0)
    shaped = present.reshape((-1,) + (1,) * (source.ndim - 1))
    return jnp.where(shaped, chosen, jnp.zeros_like(chosen))

def assemble(home_block, from_lower, from_upper, link_table, margin_width):
    sources = (from_lower, home_block, from_upper)
    slab_list = []
    for along_first in (-1, 0, 1):
        row_list = []
        for along_second in (-1, 0, 1):
            pieces = []
            for along_third in (-1, 0, 1):
                number = 9 * (along_first + 1) + 3 * (along_second + 1) + (along_third + 1)
                if number == 13:
                    region = home_block
                else:
                    position = number if number < 13 else number - 1
                    region = pick_rows(sources[along_first + 1], link_table[position])
                region = cut_side(region, 3, along_second, margin_width)
                region = cut_side(region, 4, along_third, margin_width)
                pieces.append(region)
            row_list.append(jnp.concatenate(pieces, axis=4))
        slab_list.append(jnp.concatenate(row_list, axis=3))
    return jnp.concatenate(slab_list, axis=2)

def plane_columns(flat_cells, side_len, plane_tap, negate, first_cell, stretch):
    pieces = []
    for row_tap in range(3):
        for column in range(3):
            offset = (plane_tap - 1) * side_len * side_len + (row_tap - 1) * side_len + (column - 1)
            if negate:
                offset = -offset
            pieces.append(lax.slice_in_dim(flat_cells, first_cell + offset, first_cell + offset + stretch, axis=1))
    return jnp.concatenate(pieces, axis=0)

def conv_region(flat_cells, kernel, side_len, negate):
    channels = flat_cells.shape[0]
    first_cell = side_len * side_len + side_len + 1
    stretch = side_len ** 3 - 2 * first_cell
    summed = jnp.zeros((kernel.shape[0], stretch), jnp.float32)
    for plane_tap in range(3):
        columns = plane_columns(flat_cells, side_len, plane_tap, negate, first_cell, stretch).astype(jnp.float32)
        part_kernel = kernel[:, plane_tap * 9 * channels:(plane_tap + 1) * 9 * channels].astype(jnp.float32)
        summed = summed + jnp.dot(part_kernel, columns, preferred_element_type=jnp.float32)
    spread = jnp.pad(summed, ((0, 0), (first_cell, first_cell)))
    volume = spread.reshape(-1, side_len, side_len, side_len)[:, 1:-1, 1:-1, 1:-1]
    return volume.reshape(volume.shape[0], -1)

def kernel_grad(flat_cells, inner_grad, side_len):
    channels = flat_cells.shape[0]
    margin_width = (side_len - EDGE) // 2
    first_cell = side_len * side_len + side_len + 1
    stretch = side_len ** 3 - 2 * first_cell
    grid = inner_grad.reshape(channels, EDGE, EDGE, EDGE)
    framed = jnp.pad(grid, ((0, 0), (margin_width, margin_width), (margin_width, margin_width), (margin_width, margin_width)))
    window = lax.slice_in_dim(framed.reshape(channels, -1), first_cell, first_cell + stretch, axis=1).astype(jnp.float32)
    parts = []
    for plane_tap in range(3):
        columns = plane_columns(flat_cells, side_len, plane_tap, False, first_cell, stretch).astype(jnp.float32)
        parts.append(lax.dot_general(window, columns, (((1,), (1,)), ((), ())), preferred_element_type=jnp.float32))
    return jnp.concatenate(parts, axis=1)

def flip_kernel(kernel):
    channels = kernel.shape[0]
    return kernel.reshape(channels, 27, channels).transpose(2, 1, 0).reshape(channels, 27 * channels)

def pad_field(field, link_table, margin_width):
    devices, slots_here, channels = (field.shape[0], field.shape[1], field.shape[2])
    cubes = field.reshape(devices, slots_here, channels, EDGE, EDGE, EDGE)
    empty = jnp.zeros_like(cubes[:1, :, :, :margin_width])
    lower = jnp.concatenate([empty, cubes[:-1, :, :, EDGE - margin_width:]], axis=0)
    upper = jnp.concatenate([cubes[1:, :, :, :margin_width], empty], axis=0)
    tables = link_table.reshape(26, devices, slots_here).transpose(1, 0, 2)
    padded = jax.vmap(partial(assemble, margin_width=margin_width))(cubes, lower, upper, tables)
    return padded.reshape(devices * slots_here, channels, -1)

def by_blocks(function, initial, arrays):
    brick_total = arrays[0].shape[0]
    blocked = tuple((member.reshape((brick_total // 8, 8) + member.shape[1:]) for member in arrays))

    def visit(running, block_items):
        grads, outputs = jax.vmap(function)(*block_items)
        return (running + lax.optimization_barrier(jnp.sum(grads, axis=0)), outputs)
    summed_grad, stacked = lax.scan(visit, initial, blocked)
    return (summed_grad, tuple((piece_out.reshape((brick_total,) + piece_out.shape[2:]) for piece_out in stacked)))

def reference(features, cotangent, brick_count, destination, neighbours, kernel_one, kernel_two):
    channels = features.shape[2]
    flip_one = flip_kernel(kernel_one)
    flip_two = flip_kernel(kernel_two)
    side_len = EDGE + 2
    zero_grad = jnp.zeros((channels, 27 * channels), jnp.float32)

    def one_volume(totals, inputs):
        volume_features, volume_cots, counts, dests, links = inputs
        devices = counts.shape[0]
        slot_ids = jnp.arange(HOME_CAP, dtype=jnp.int32)
        active = (slot_ids[None, :] < counts[:, None]).reshape(-1)
        keep = active[:, None, None]
        masked_x = jnp.where(keep, volume_features, jnp.zeros_like(volume_features))
        masked_dy = jnp.where(keep, volume_cots, jnp.zeros_like(volume_cots))
        shaped = (devices, HOME_CAP, channels, CELLS)
        padded_x = pad_field(masked_x.reshape(shaped), links, 1)

        def first_section(cells_x):
            pre = conv_region(cells_x, kernel_one, side_len, False)
            return (zero_grad, (pre, jax.nn.silu(pre).astype(jnp.bfloat16)))
        unused_grad, (pre_all, hidden_all) = by_blocks(first_section, zero_grad, (padded_x,))
        hidden_all = jnp.where(keep, hidden_all, jnp.zeros_like(hidden_all))
        padded_h = pad_field(hidden_all.reshape(shaped), links, 1)
        padded_dy = pad_field(masked_dy.reshape(shaped), links, 1)

        def second_section(cells_h, cells_dy, inner_x, inner_dy, pre):
            mixed = conv_region(cells_h, kernel_two, side_len, False)
            out_brick = (inner_x.astype(jnp.float32) + mixed).astype(jnp.bfloat16)
            grad_hidden = conv_region(cells_dy, flip_two, side_len, True)
            sigma = jax.nn.sigmoid(pre)
            grad_pre = (grad_hidden * (sigma * (1.0 + pre * (1.0 - sigma)))).astype(jnp.bfloat16)
            return (kernel_grad(cells_h, inner_dy, side_len), (out_brick, grad_pre))
        grad_two, (out_all, grad_pre_all) = by_blocks(second_section, zero_grad, (padded_h, padded_dy, masked_x, masked_dy, pre_all))
        out_all = jnp.where(keep, out_all, jnp.zeros_like(out_all))
        grad_pre_all = jnp.where(keep, grad_pre_all, jnp.zeros_like(grad_pre_all))
        padded_g = pad_field(grad_pre_all.reshape(shaped), links, 1)

        def third_section(cells_g, cells_x, inner_g, inner_dy):
            back_term = conv_region(cells_g, flip_one, side_len, True).astype(jnp.bfloat16)
            summed = (inner_dy.astype(jnp.float32) + back_term.astype(jnp.float32)).astype(jnp.bfloat16)
            return (kernel_grad(cells_x, inner_g, side_len), (summed,))
        grad_one, (grad_in,) = by_blocks(third_section, zero_grad, (padded_g, padded_x, grad_pre_all, masked_dy))
        grad_in = jnp.where(keep, grad_in, jnp.zeros_like(grad_in))
        works = devices * WORK_CAP
        targets = jnp.where(active, dests, works).astype(jnp.int32)
        placed = jnp.zeros((works, channels, CELLS), out_all.dtype).at[targets].set(out_all, mode='drop')
        return ((totals[0] + grad_one, totals[1] + grad_two), (placed, grad_in))
    (grad_one, grad_two), (block_output, grad_features) = lax.scan(one_volume, (zero_grad, zero_grad), (features, cotangent, brick_count, destination, neighbours))
    scale = 1.0 / math.sqrt(GROUPS * SLOTS * CELLS)
    return (block_output, grad_features, grad_one * scale, grad_two * scale)
```

```python
import math

import jax
import jax.numpy as jnp
import numpy as np
from jax import lax
from jax.experimental import pallas as pl
from jax.experimental.pallas import tpu as pltpu
from jax.sharding import PartitionSpec as P

EDGE = 8
WORK_CAP = 2
CELLS = EDGE**3
PLANE = EDGE * EDGE
LONG = CELLS + 2 * PLANE
LANES = 128
SIDES = (-1, 0, 1)
RING = [(q, r) for q in SIDES for r in SIDES]
TURNS = [(q, r) for q, r in RING if (q, r) != (0, 0)]


def turn_tables():
    cell = np.arange(PLANE)
    row, column = cell // EDGE, cell % EDGE
    moves = np.zeros((len(TURNS), 4 * PLANE, 4 * PLANE), np.float32)
    for number, (q, r) in enumerate(TURNS):
        source = ((row + q) % EDGE) * EDGE + (column + r) % EDGE
        for block in range(4):
            moves[number, block * PLANE + source, block * PLANE + cell] = 1
    lane = np.arange(LONG) % PLANE
    edges = np.stack(
        [
            lane // EDGE == EDGE - 1,
            lane // EDGE == 0,
            lane % EDGE == EDGE - 1,
            lane % EDGE == 0,
        ]
    ).astype(np.float32)
    edges = np.broadcast_to(edges[:, None, :], (4, 16, LONG))
    return jnp.asarray(moves, jnp.bfloat16), jnp.asarray(edges, jnp.bfloat16)


def shifted_right(values):
    tail = jnp.zeros((values.shape[0], LONG - CELLS), jnp.float32)
    return pltpu.roll(jnp.concatenate([values, tail], axis=1), PLANE, 1)


def stage(x_ref, dy_ref, long_ref, last_ref, first_ref):
    slots, channels = x_ref.shape[0], x_ref.shape[1]
    for slot in range(slots):
        for half, ref in enumerate((x_ref, dy_ref)):
            long_ref[slot, half * channels : (half + 1) * channels, :] = shifted_right(
                ref[slot].astype(jnp.float32)
            ).astype(jnp.bfloat16)
        last_ref[slot] = long_ref[slot, :, LONG - LANES :]
        first_ref[slot] = long_ref[slot, :, :LANES]
    long_ref[slots] = jnp.zeros(long_ref.shape[1:], jnp.bfloat16)


def gather_sides(slots, low_ref, high_ref, low, high):
    for slot in range(slots):
        low[slot] = low_ref[slot]
        high[slot] = high_ref[slot]
    low[slots] = jnp.zeros(low.shape[1:], jnp.bfloat16)
    high[slots] = jnp.zeros(high.shape[1:], jnp.bfloat16)


def spread(j, slots, link, long_ref, low, high, edge_ref, move_ref, mixed, outs):
    rows = long_ref.shape[1]
    channels = rows // 2
    place = {}
    for p in SIDES:
        for q, r in RING:
            if (p, q, r) == (0, 0, 0):
                place[p, q, r] = j
                continue
            number = 9 * (p + 1) + 3 * (q + 1) + (r + 1)
            number = number if number < 13 else number - 1
            found = link[number * slots + j]
            place[p, q, r] = jnp.where(found < 0, slots, found)
    one = jnp.ones((16, LANES), jnp.bfloat16)
    for tile in range(LONG // LANES):
        span = slice(tile * LANES, (tile + 1) * LANES)
        edge = {
            name: edge_ref[k, :, span]
            for k, name in enumerate((("q", -1), ("q", 1), ("r", -1), ("r", 1)))
        }
        inner = {name: one - value for name, value in edge.items()}
        for part in range(rows // 16):
            band = slice(part * 16, (part + 1) * 16)
            raw = {}
            for q, r in RING:
                value = long_ref[place[0, q, r], band, span]
                if tile == 0:
                    value = value + low[place[-1, q, r], band, :]
                if tile == LONG // LANES - 1:
                    value = value + high[place[1, q, r], band, :]
                raw[q, r] = value
            for r in (-1, 1):
                for q in SIDES:
                    raw[q, r] = raw[q, 0] * inner["r", r] + raw[q, r] * edge["r", r]
            for number, (q, r) in enumerate(TURNS):
                value = raw[q, r]
                if q != 0:
                    value = raw[0, r] * inner["q", q] + raw[q, r] * edge["q", q]
                mixed[number, band, span] = value
            half, start = divmod(part * 16, channels)
            start += 4 * channels
            outs[half][start : start + 16, span] = raw[0, 0]
    for number, (q, r) in enumerate(TURNS):
        start = RING.index((q, r)) * channels
        for low_lane in range(0, LONG, 4 * PLANE):
            width = min(4 * PLANE, LONG - low_lane)
            moved = jnp.dot(
                mixed[number, :, low_lane : low_lane + width],
                move_ref[number, :width, :width],
                preferred_element_type=jnp.float32,
            ).astype(jnp.bfloat16)
            for half in range(2):
                outs[half][start : start + channels, low_lane : low_lane + width] = moved[
                    half * channels : (half + 1) * channels
                ]


def convolved(weight_ref, field):
    channels = weight_ref.shape[0] // 3
    parts = jnp.dot(weight_ref[...], field[...], preferred_element_type=jnp.float32)
    middle = pltpu.roll(parts[channels : 2 * channels], LONG - PLANE, 1)
    return (
        parts[:channels, :CELLS] + middle[:, :CELLS] + parts[2 * channels :, LONG - CELLS :]
    )


def three_ways(values, moved):
    tail = jnp.zeros((values.shape[0], LONG - CELLS), jnp.float32)
    return jnp.concatenate(
        [
            jnp.concatenate([values, tail], axis=1).astype(jnp.bfloat16),
            moved,
            jnp.concatenate([tail, values], axis=1).astype(jnp.bfloat16),
        ],
        axis=0,
    )


def first_half(
    link, count, long_ref, low_ref, high_ref, edge_ref, move_ref, one_ref, two_ref,
    inner_ref, last_ref, first_ref, grad_ref,
    low, high, mixed, field_x, field_dy, sum_one, sum_two,
):
    slots = low_ref.shape[0]
    channels = long_ref.shape[1] // 2
    gather_sides(slots, low_ref, high_ref, low, high)
    sum_one[...] = jnp.zeros_like(sum_one)
    sum_two[...] = jnp.zeros_like(sum_two)
    inner_ref[...] = jnp.zeros_like(inner_ref)

    def visit(j, carry):
        spread(
            j, slots, link, long_ref, low, high, edge_ref, move_ref, mixed, (field_x, field_dy)
        )
        pre = convolved(one_ref, field_x)
        grad_hidden = convolved(two_ref, field_dy)
        sigma = 1.0 / (1.0 + jnp.exp(-pre))
        hidden = pre * sigma
        grad_pre = grad_hidden * (sigma * (1.0 + pre * (1.0 - sigma)))
        hidden_long = shifted_right(hidden).astype(jnp.bfloat16)
        grad_long = shifted_right(grad_pre).astype(jnp.bfloat16)
        inner_ref[j, :channels, :] = hidden_long
        inner_ref[j, channels:, :] = grad_long
        sum_one[...] += lax.dot_general(
            three_ways(grad_pre, grad_long),
            field_x[...],
            (((1,), (1,)), ((), ())),
            preferred_element_type=jnp.float32,
        )
        sum_two[...] += lax.dot_general(
            field_dy[...],
            three_ways(hidden, hidden_long),
            (((1,), (1,)), ((), ())),
            preferred_element_type=jnp.float32,
        )
        return carry

    lax.fori_loop(0, count[0], visit, 0)
    for slot in range(slots):
        last_ref[slot] = inner_ref[slot, :, LONG - LANES :]
        first_ref[slot] = inner_ref[slot, :, :LANES]
    grad_ref[:channels, :] = jnp.concatenate(
        [sum_one[p * channels : (p + 1) * channels, :] for p in range(3)], axis=1
    )
    blocks = []
    for tap in range(27):
        p, rest = divmod(26 - tap, 9)
        blocks.append(
            sum_two[rest * channels : (rest + 1) * channels, p * channels : (p + 1) * channels]
        )
    grad_ref[channels:, :] = jnp.concatenate(blocks, axis=1)


def second_half(
    link, count, inner_ref, low_ref, high_ref, edge_ref, move_ref, two_ref, one_ref, x_ref, dy_ref,
    out_ref, back_ref,
    low, high, mixed, field_h, field_g,
):
    slots = low_ref.shape[0]
    gather_sides(slots, low_ref, high_ref, low, high)
    out_ref[...] = jnp.zeros_like(out_ref)
    back_ref[...] = jnp.zeros_like(back_ref)

    def visit(j, carry):
        spread(
            j, slots, link, inner_ref, low, high, edge_ref, move_ref, mixed, (field_h, field_g)
        )
        out = convolved(two_ref, field_h)
        back = convolved(one_ref, field_g).astype(jnp.bfloat16)
        out_ref[j] = (x_ref[j].astype(jnp.float32) + out).astype(jnp.bfloat16)
        back_ref[j] = (dy_ref[j].astype(jnp.float32) + back.astype(jnp.float32)).astype(
            jnp.bfloat16
        )
        return carry

    lax.fori_loop(0, count[0], visit, 0)


def vmem(count):
    return [pl.BlockSpec(memory_space=pltpu.VMEM)] * count


def smem(count):
    return [pl.BlockSpec(memory_space=pltpu.SMEM)] * count


def step_to(x, by, wrap):
    size = lax.axis_size("space")
    pairs = [(i, (i + by) % size) for i in range(size) if wrap or 0 <= i + by < size]
    return lax.ppermute(x, "space", pairs)


def all_sum(rows):
    levels = []
    for axis in ("space", "batch"):
        reach = 1
        while reach < lax.axis_size(axis):
            levels.append((axis, reach))
            reach *= 2

    def swap(value, axis, reach):
        size = lax.axis_size(axis)
        return lax.ppermute(value, axis, [(i, i ^ reach) for i in range(size)])

    taken = []
    for number, (axis, reach) in enumerate(levels):
        wire = jnp.float32 if number == 0 or rows.shape[0] <= 16 else jnp.bfloat16
        if rows.shape[0] > 8:
            upper = (lax.axis_index(axis) // reach) % 2 == 1
            middle = rows.shape[0] // 2
            keep = jnp.where(upper, rows[middle:], rows[:middle])
            give = jnp.where(upper, rows[:middle], rows[middle:]).astype(wire)
            rows = keep + swap(give, axis, reach).astype(jnp.float32)
            taken.append((axis, reach, upper))
        else:
            rows = rows + swap(rows, axis, reach)
    rows = rows.astype(jnp.bfloat16)
    for axis, reach, upper in taken[::-1]:
        other = swap(rows, axis, reach)
        rows = jnp.concatenate(
            [jnp.where(upper, other, rows), jnp.where(upper, rows, other)], axis=0
        )
    return rows


def shards(features, cotangent, brick_count, destination, neighbours, kernel_one, kernel_two):
    slots, channels = features.shape[1], features.shape[2]
    taps = kernel_one.shape[1] // channels
    x, dy = features[0], cotangent[0]
    count = brick_count[0]
    link = neighbours[0].reshape(-1)
    bf16, f32 = jnp.bfloat16, jnp.float32
    shape = jax.ShapeDtypeStruct
    long_shape = shape((slots + 1, 2 * channels, LONG), bf16)
    side_shape = shape((slots, 2 * channels, LANES), bf16)
    moves, edges = turn_tables()

    def straight(kernel):
        return (
            kernel.reshape(channels, 3, 9 * channels)
            .transpose(1, 0, 2)
            .reshape(3 * channels, 9 * channels)
        )

    def turned(kernel):
        return (
            kernel.reshape(channels, taps, channels)[:, ::-1]
            .reshape(channels, 3, 9, channels)
            .transpose(1, 3, 2, 0)
            .reshape(3 * channels, 9 * channels)
        )

    long_in, last, first = pl.pallas_call(
        stage,
        out_shape=(long_shape, side_shape, side_shape),
        in_specs=vmem(2),
        out_specs=tuple(vmem(3)),
        name="stage",
    )(x, dy)
    low = step_to(last, 1, False)
    high = step_to(first, -1, False)
    side_scratch = pltpu.VMEM((slots + 1, 2 * channels, LANES), bf16)
    mixed_scratch = pltpu.VMEM((len(TURNS), 2 * channels, LONG), bf16)
    field_scratch = pltpu.VMEM((9 * channels, LONG), bf16)
    inner, inner_last, inner_first, grads = pl.pallas_call(
        first_half,
        out_shape=(
            long_shape,
            side_shape,
            side_shape,
            shape((2 * channels, taps * channels), f32),
        ),
        in_specs=smem(2) + vmem(7),
        out_specs=tuple(vmem(4)),
        scratch_shapes=[
            side_scratch,
            side_scratch,
            mixed_scratch,
            field_scratch,
            field_scratch,
            pltpu.VMEM((3 * channels, 9 * channels), f32),
            pltpu.VMEM((9 * channels, 3 * channels), f32),
        ],
        name="first_half",
    )(link, count, long_in, low, high, edges, moves, straight(kernel_one), turned(kernel_two))
    inner_low = step_to(inner_last, 1, False)
    inner_high = step_to(inner_first, -1, False)
    out, grad_in = pl.pallas_call(
        second_half,
        out_shape=(shape(x.shape, bf16), shape(x.shape, bf16)),
        in_specs=smem(2) + vmem(9),
        out_specs=tuple(vmem(2)),
        scratch_shapes=[side_scratch, side_scratch, mixed_scratch, field_scratch, field_scratch],
        name="second_half",
    )(
        link, count, inner, inner_low, inner_high, edges, moves,
        straight(kernel_two), turned(kernel_one), x, dy,
    )
    arrived = jnp.zeros_like(out[0])
    for step in range(slots - WORK_CAP):
        arrived = arrived + step_to(out[WORK_CAP + step], step + 1, True)
    free = (jnp.arange(WORK_CAP, dtype=jnp.int32) == count[0])[:, None, None]
    placed = jnp.where(free, arrived[None], out[:WORK_CAP])
    scale = 1.0 / math.sqrt(
        lax.axis_size("batch") * features.shape[0] * lax.axis_size("space") * slots * CELLS
    )
    total = all_sum(grads).astype(f32) * scale
    return (placed[None], grad_in[None], total[:channels], total[channels:])


def solution(mesh):
    return jax.shard_map(
        shards,
        mesh=mesh,
        in_specs=(
            P("batch", "space", None, None),
            P("batch", "space", None, None),
            P("batch", "space"),
            P("batch", "space"),
            P("batch", None, "space"),
            P(),
            P(),
        ),
        out_specs=(P("batch", "space", None, None), P("batch", "space", None, None), P(), P()),
        check_vma=False,
    )
```

```python
import math

import jax
import jax.numpy as jnp
import numpy as np
from jax import lax
from jax.experimental import pallas as pl
from jax.experimental.pallas import tpu as pltpu
from jax.sharding import PartitionSpec as P


EDGE = 8
WORK_CAP = 2
CELLS = EDGE**3
PLANE = EDGE * EDGE
LONG = CELLS + 2 * PLANE
LANES = 128
SIDES = (-1, 0, 1)
RING = [(q, r) for q in SIDES for r in SIDES]
TURNS = [(q, r) for q, r in RING if (q, r) != (0, 0)]


def turn_tables():
    cell = np.arange(PLANE)
    row, column = cell // EDGE, cell % EDGE
    moves = np.zeros((len(TURNS), 4 * PLANE, 4 * PLANE), np.float32)
    for number, (q, r) in enumerate(TURNS):
        source = ((row + q) % EDGE) * EDGE + (column + r) % EDGE
        for block in range(4):
            moves[number, block * PLANE + source, block * PLANE + cell] = 1
    lane = np.arange(LONG) % PLANE
    edges = np.stack(
        [
            lane // EDGE == EDGE - 1,
            lane // EDGE == 0,
            lane % EDGE == EDGE - 1,
            lane % EDGE == 0,
        ]
    ).astype(np.float32)
    edges = np.broadcast_to(edges[:, None, :], (4, 16, LONG))
    return jnp.asarray(moves, jnp.bfloat16), jnp.asarray(edges, jnp.bfloat16)


def shifted_right(values):
    tail = jnp.zeros((values.shape[0], LONG - CELLS), jnp.float32)
    return pltpu.roll(jnp.concatenate([values, tail], axis=1), PLANE, 1)


def sides(x_first, x_last, dy_first, dy_last, last_ref, first_ref):
    slots, channels = x_first.shape[0], x_first.shape[1]
    front = lax.broadcasted_iota(jnp.int32, (channels, LANES), 1) < PLANE
    for slot in range(slots):
        for half, (begin, end) in enumerate(((x_first, x_last), (dy_first, dy_last))):
            band = slice(half * channels, (half + 1) * channels)
            late = pltpu.roll(end[slot].astype(jnp.float32), PLANE, 1)
            last_ref[slot, band, :] = jnp.where(front, late, 0.0).astype(jnp.bfloat16)
            early = pltpu.roll(begin[slot].astype(jnp.float32), PLANE, 1)
            first_ref[slot, band, :] = jnp.where(front, 0.0, early).astype(jnp.bfloat16)


def prepare(
    x_ref, dy_ref, one_ref, two_ref, long_ref, one_straight, two_straight, one_turned, two_turned
):
    slots, channels = x_ref.shape[0], x_ref.shape[1]
    for slot in range(slots):
        for half, ref in enumerate((x_ref, dy_ref)):
            long_ref[slot, half * channels : (half + 1) * channels, :] = shifted_right(
                ref[slot].astype(jnp.float32)
            ).astype(jnp.bfloat16)
    long_ref[slots] = jnp.zeros(long_ref.shape[1:], jnp.bfloat16)
    width = one_ref.shape[1]
    third = width // 3
    both = jnp.concatenate(
        [one_ref[...].astype(jnp.float32), two_ref[...].astype(jnp.float32)], axis=0
    )
    for p in range(3):
        part = both[:, p * third : (p + 1) * third].astype(jnp.bfloat16)
        one_straight[p * channels : (p + 1) * channels, :] = part[:channels]
        two_straight[p * channels : (p + 1) * channels, :] = part[channels:]
    taps = width // channels
    spare = -width % LANES
    flipped = jnp.concatenate([both, jnp.zeros((2 * channels, spare), jnp.float32)], axis=1).T
    front = lax.broadcasted_iota(jnp.int32, (channels, LANES), 1) < PLANE

    def block(tap):
        return flipped[tap * channels : (tap + 1) * channels, :]

    for p in range(3):
        band = slice(p * channels, (p + 1) * channels)
        for start in range(0, 9, 2):
            here = block(taps - 1 - (9 * p + start))
            lanes = slice(start * channels, min(start + 2, 9) * channels)
            if start + 1 < 9:
                after = block(taps - 1 - (9 * p + start + 1))
                one = jnp.where(front, here, pltpu.roll(after, PLANE, 1))
                two = jnp.where(front, pltpu.roll(here, PLANE, 1), after)
            else:
                one, two = here[:, :channels], pltpu.roll(here, PLANE, 1)[:, :channels]
            one_turned[band, lanes] = one.astype(jnp.bfloat16)
            two_turned[band, lanes] = two.astype(jnp.bfloat16)


def gather_sides(slots, low_ref, high_ref, low, high):
    for slot in range(slots):
        low[slot] = low_ref[slot]
        high[slot] = high_ref[slot]
    low[slots] = jnp.zeros(low.shape[1:], jnp.bfloat16)
    high[slots] = jnp.zeros(high.shape[1:], jnp.bfloat16)


def spread(j, slots, link, long_ref, low, high, edge_ref, move_ref, mixed, outs):
    rows = long_ref.shape[1]
    channels = rows // 2
    place = {}
    for p in SIDES:
        for q, r in RING:
            if (p, q, r) == (0, 0, 0):
                place[p, q, r] = j
                continue
            number = 9 * (p + 1) + 3 * (q + 1) + (r + 1)
            number = number if number < 13 else number - 1
            found = link[j, number]
            place[p, q, r] = jnp.where(found < 0, slots, found)
    one = jnp.ones((16, LANES), jnp.bfloat16)
    for tile in range(LONG // LANES):
        span = slice(tile * LANES, (tile + 1) * LANES)
        edge = {
            name: edge_ref[k, :, span]
            for k, name in enumerate((("q", -1), ("q", 1), ("r", -1), ("r", 1)))
        }
        inner = {name: one - value for name, value in edge.items()}
        for part in range(rows // 16):
            band = slice(part * 16, (part + 1) * 16)
            raw = {}
            for q, r in RING:
                value = long_ref[place[0, q, r], band, span]
                if tile == 0:
                    value = value + low[place[-1, q, r], band, :]
                if tile == LONG // LANES - 1:
                    value = value + high[place[1, q, r], band, :]
                raw[q, r] = value
            for r in (-1, 1):
                for q in SIDES:
                    raw[q, r] = raw[q, 0] * inner["r", r] + raw[q, r] * edge["r", r]
            for number, (q, r) in enumerate(TURNS):
                value = raw[q, r]
                if q != 0:
                    value = raw[0, r] * inner["q", q] + raw[q, r] * edge["q", q]
                mixed[number, band, span] = value
            half, start = divmod(part * 16, channels)
            start += 4 * channels
            outs[half][start : start + 16, span] = raw[0, 0]
    for number, (q, r) in enumerate(TURNS):
        start = RING.index((q, r)) * channels
        for low_lane in range(0, LONG, 4 * PLANE):
            width = min(4 * PLANE, LONG - low_lane)
            moved = jnp.dot(
                mixed[number, :, low_lane : low_lane + width],
                move_ref[number, :width, :width],
                preferred_element_type=jnp.float32,
            ).astype(jnp.bfloat16)
            for half in range(2):
                outs[half][start : start + channels, low_lane : low_lane + width] = moved[
                    half * channels : (half + 1) * channels
                ]


def convolved(weight_ref, field):
    channels = weight_ref.shape[0] // 3
    parts = jnp.dot(weight_ref[...], field[...], preferred_element_type=jnp.float32)
    middle = pltpu.roll(parts[channels : 2 * channels], LONG - PLANE, 1)
    return (
        parts[:channels, :CELLS] + middle[:, :CELLS] + parts[2 * channels :, LONG - CELLS :]
    )


def three_ways(values, moved):
    tail = jnp.zeros((values.shape[0], LONG - CELLS), jnp.float32)
    return jnp.concatenate(
        [
            jnp.concatenate([values, tail], axis=1).astype(jnp.bfloat16),
            moved,
            jnp.concatenate([tail, values], axis=1).astype(jnp.bfloat16),
        ],
        axis=0,
    )


def first_half(
    link, count, long_ref, low_ref, high_ref, edge_ref, move_ref, one_ref, two_ref,
    inner_ref, last_ref, first_ref, grad_ref,
    low, high, mixed, field_x, field_dy, sum_one, sum_two,
):
    slots = low_ref.shape[0]
    channels = long_ref.shape[1] // 2
    gather_sides(slots, low_ref, high_ref, low, high)
    sum_one[...] = jnp.zeros_like(sum_one)
    sum_two[...] = jnp.zeros_like(sum_two)
    inner_ref[...] = jnp.zeros_like(inner_ref)

    def visit(j, carry):
        spread(
            j, slots, link, long_ref, low, high, edge_ref, move_ref, mixed, (field_x, field_dy)
        )
        pre = convolved(one_ref, field_x)
        grad_hidden = convolved(two_ref, field_dy)
        sigma = 1.0 / (1.0 + jnp.exp(-pre))
        hidden = pre * sigma
        grad_pre = grad_hidden * (sigma * (1.0 + pre * (1.0 - sigma)))
        hidden_long = shifted_right(hidden).astype(jnp.bfloat16)
        grad_long = shifted_right(grad_pre).astype(jnp.bfloat16)
        inner_ref[j, :channels, :] = hidden_long
        inner_ref[j, channels:, :] = grad_long
        sum_one[...] += lax.dot_general(
            three_ways(grad_pre, grad_long),
            field_x[...],
            (((1,), (1,)), ((), ())),
            preferred_element_type=jnp.float32,
        )
        sum_two[...] += lax.dot_general(
            field_dy[...],
            three_ways(hidden, hidden_long),
            (((1,), (1,)), ((), ())),
            preferred_element_type=jnp.float32,
        )
        return carry

    lax.fori_loop(0, count[0], visit, 0)
    for slot in range(slots):
        last_ref[slot] = inner_ref[slot, :, LONG - LANES :]
        first_ref[slot] = inner_ref[slot, :, :LANES]
    grad_ref[:channels, :] = jnp.concatenate(
        [sum_one[p * channels : (p + 1) * channels, :] for p in range(3)], axis=1
    )
    blocks = []
    for tap in range(27):
        p, rest = divmod(26 - tap, 9)
        blocks.append(
            sum_two[rest * channels : (rest + 1) * channels, p * channels : (p + 1) * channels]
        )
    grad_ref[channels:, :] = jnp.concatenate(blocks, axis=1)


def second_half(
    link, count, inner_ref, low_ref, high_ref, edge_ref, move_ref, two_ref, one_ref, x_ref, dy_ref,
    out_ref, back_ref,
    low, high, mixed, field_h, field_g,
):
    slots = low_ref.shape[0]
    gather_sides(slots, low_ref, high_ref, low, high)
    out_ref[...] = jnp.zeros_like(out_ref)
    back_ref[...] = jnp.zeros_like(back_ref)

    def visit(j, carry):
        spread(
            j, slots, link, inner_ref, low, high, edge_ref, move_ref, mixed, (field_h, field_g)
        )
        out = convolved(two_ref, field_h)
        back = convolved(one_ref, field_g).astype(jnp.bfloat16)
        out_ref[j] = (x_ref[j].astype(jnp.float32) + out).astype(jnp.bfloat16)
        back_ref[j] = (dy_ref[j].astype(jnp.float32) + back.astype(jnp.float32)).astype(
            jnp.bfloat16
        )
        return carry

    lax.fori_loop(0, count[0], visit, 0)


def vmem(count):
    return [pl.BlockSpec(memory_space=pltpu.VMEM)] * count


def smem(count):
    return [pl.BlockSpec(memory_space=pltpu.SMEM)] * count


def step_to(x, by, wrap):
    size = lax.axis_size("space")
    pairs = [(i, (i + by) % size) for i in range(size) if wrap or 0 <= i + by < size]
    return lax.ppermute(x, "space", pairs)


def all_sum(rows):
    levels = []
    for axis in ("space", "batch"):
        reach = 1
        while reach < lax.axis_size(axis):
            levels.append((axis, reach))
            reach *= 2

    def swap(value, axis, reach):
        size = lax.axis_size(axis)
        return lax.ppermute(value, axis, [(i, i ^ reach) for i in range(size)])

    taken = []
    for number, (axis, reach) in enumerate(levels):
        wire = jnp.float32 if number == 0 or rows.shape[0] <= 16 else jnp.bfloat16
        if rows.shape[0] > 8:
            upper = (lax.axis_index(axis) // reach) % 2 == 1
            middle = rows.shape[0] // 2
            keep = jnp.where(upper, rows[middle:], rows[:middle])
            give = jnp.where(upper, rows[:middle], rows[middle:]).astype(wire)
            rows = keep + swap(give, axis, reach).astype(jnp.float32)
            taken.append((axis, reach, upper))
        else:
            rows = rows + swap(rows, axis, reach)
    rows = rows.astype(jnp.bfloat16)
    for axis, reach, upper in taken[::-1]:
        other = swap(rows, axis, reach)
        rows = jnp.concatenate(
            [jnp.where(upper, other, rows), jnp.where(upper, rows, other)], axis=0
        )
    return rows


def shards(features, cotangent, brick_count, destination, neighbours, kernel_one, kernel_two):
    slots, channels = features.shape[1], features.shape[2]
    taps = kernel_one.shape[1] // channels
    x, dy = features[0], cotangent[0]
    count = brick_count[0]
    link = neighbours[0].T
    bf16, f32 = jnp.bfloat16, jnp.float32
    shape = jax.ShapeDtypeStruct
    long_shape = shape((slots + 1, 2 * channels, LONG), bf16)
    side_shape = shape((slots, 2 * channels, LANES), bf16)
    moves, edges = turn_tables()
    params = pltpu.CompilerParams(vmem_limit_bytes=20 * 2**20)

    ends = [pl.BlockSpec((slots, channels, LANES), lambda i, at=at: (0, 0, at)) for at in (0, 3)]
    whole = pl.BlockSpec((slots, 2 * channels, LANES), lambda i: (0, 0, 0))
    last, first = pl.pallas_call(
        sides,
        grid=(1,),
        out_shape=(side_shape, side_shape),
        in_specs=ends + ends,
        out_specs=(whole, whole),
        compiler_params=params,
        name="sides",
    )(x, x, dy, dy)
    weight_shape = shape((3 * channels, 9 * channels), bf16)
    long_in, one_straight, two_straight, one_turned, two_turned = pl.pallas_call(
        prepare,
        out_shape=(long_shape,) + (weight_shape,) * 4,
        in_specs=vmem(4),
        out_specs=tuple(vmem(5)),
        compiler_params=params,
        name="prepare",
    )(x, dy, kernel_one, kernel_two)
    low = step_to(last, 1, False)
    high = step_to(first, -1, False)
    side_scratch = pltpu.VMEM((slots + 1, 2 * channels, LANES), bf16)
    mixed_scratch = pltpu.VMEM((len(TURNS), 2 * channels, LONG), bf16)
    field_scratch = pltpu.VMEM((9 * channels, LONG), bf16)
    inner, inner_last, inner_first, grads = pl.pallas_call(
        first_half,
        out_shape=(
            long_shape,
            side_shape,
            side_shape,
            shape((2 * channels, taps * channels), f32),
        ),
        in_specs=smem(2) + vmem(7),
        out_specs=tuple(vmem(4)),
        scratch_shapes=[
            side_scratch,
            side_scratch,
            mixed_scratch,
            field_scratch,
            field_scratch,
            pltpu.VMEM((3 * channels, 9 * channels), f32),
            pltpu.VMEM((9 * channels, 3 * channels), f32),
        ],
        compiler_params=params,
        name="first_half",
    )(link, count, long_in, low, high, edges, moves, one_straight, two_turned)
    inner_low = step_to(inner_last, 1, False)
    inner_high = step_to(inner_first, -1, False)
    out, grad_in = pl.pallas_call(
        second_half,
        out_shape=(shape(x.shape, bf16), shape(x.shape, bf16)),
        in_specs=smem(2) + vmem(9),
        out_specs=tuple(vmem(2)),
        scratch_shapes=[side_scratch, side_scratch, mixed_scratch, field_scratch, field_scratch],
        compiler_params=params,
        name="second_half",
    )(
        link, count, inner, inner_low, inner_high, edges, moves, two_straight, one_turned, x, dy
    )
    arrived = jnp.zeros_like(out[0])
    for step in range(slots - WORK_CAP):
        arrived = arrived + step_to(out[WORK_CAP + step], step + 1, True)
    free = (jnp.arange(WORK_CAP, dtype=jnp.int32) == count[0])[:, None, None]
    placed = jnp.where(free, arrived[None], out[:WORK_CAP])
    scale = 1.0 / math.sqrt(
        lax.axis_size("batch") * features.shape[0] * lax.axis_size("space") * slots * CELLS
    )
    total = all_sum(grads).astype(f32) * scale
    return (placed[None], grad_in[None], total[:channels], total[channels:])


def solution(mesh):
    return whole_step(mesh, shards)


def whole_step(mesh, step):
    return jax.shard_map(
        step,
        mesh=mesh,
        in_specs=(
            P("batch", "space", None, None),
            P("batch", "space", None, None),
            P("batch", "space"),
            P("batch", "space"),
            P("batch", None, "space"),
            P(),
            P(),
        ),
        out_specs=(P("batch", "space", None, None), P("batch", "space", None, None), P(), P()),
        check_vma=False,
    )
```

```python
import math
from functools import partial

import jax
import jax.numpy as jnp
import numpy as np
from jax import lax
from jax.experimental import pallas as pl
from jax.experimental.pallas import tpu as pltpu
from jax.sharding import PartitionSpec as P


EDGE = 8
WORK_CAP = 2
CELLS = EDGE**3
PLANE = EDGE * EDGE
LONG = CELLS + 2 * PLANE
LANES = 128
SIDES = (-1, 0, 1)
RING = [(q, r) for q in SIDES for r in SIDES]
TURNS = [(q, r) for q, r in RING if (q, r) != (0, 0)]


def turn_tables():
    cell = np.arange(PLANE)
    row, column = cell // EDGE, cell % EDGE
    moves = np.zeros((len(TURNS), 4 * PLANE, 4 * PLANE), np.float32)
    for number, (q, r) in enumerate(TURNS):
        source = ((row + q) % EDGE) * EDGE + (column + r) % EDGE
        for block in range(4):
            moves[number, block * PLANE + source, block * PLANE + cell] = 1
    lane = np.arange(LONG) % PLANE
    edges = np.stack(
        [
            lane // EDGE == EDGE - 1,
            lane // EDGE == 0,
            lane % EDGE == EDGE - 1,
            lane % EDGE == 0,
        ]
    ).astype(np.float32)
    edges = np.broadcast_to(edges[:, None, :], (4, 16, LONG))
    return jnp.asarray(moves, jnp.bfloat16), jnp.asarray(edges, jnp.bfloat16)


def shifted_right(values):
    tail = jnp.zeros((values.shape[0], LONG - CELLS), jnp.float32)
    return pltpu.roll(jnp.concatenate([values, tail], axis=1), PLANE, 1)


def sides(x_ref, dy_ref, last_ref, first_ref, begin, end, sems):
    slots, channels = x_ref.shape[0], x_ref.shape[1]
    copies = []
    for half, ref in enumerate((x_ref, dy_ref)):
        for number, (box, at) in enumerate(((begin, 0), (end, CELLS - LANES))):
            copies.append(
                pltpu.make_async_copy(
                    ref.at[:, :, pl.ds(at, LANES)], box.at[half], sems.at[half, number]
                )
            )
    for copy in copies:
        copy.start()
    for copy in copies:
        copy.wait()
    front = lax.broadcasted_iota(jnp.int32, (channels, LANES), 1) < PLANE
    for slot in range(slots):
        for half in range(2):
            band = slice(half * channels, (half + 1) * channels)
            late = pltpu.roll(end[half, slot].astype(jnp.float32), PLANE, 1)
            last_ref[slot, band, :] = jnp.where(front, late, 0.0).astype(jnp.bfloat16)
            early = pltpu.roll(begin[half, slot].astype(jnp.float32), PLANE, 1)
            first_ref[slot, band, :] = jnp.where(front, 0.0, early).astype(jnp.bfloat16)


def prepare(
    x_far, dy_far, one_far, two_far,
    long_ref, one_straight, two_straight, one_turned, two_turned,
    x_ref, dy_ref, one_ref, two_ref, sems,
):
    pairs = ((x_far, x_ref), (dy_far, dy_ref), (one_far, one_ref), (two_far, two_ref))
    copies = [
        pltpu.make_async_copy(far, near, sems.at[k]) for k, (far, near) in enumerate(pairs)
    ]
    for copy in copies:
        copy.start()
    for copy in copies:
        copy.wait()
    slots, channels = x_ref.shape[0], x_ref.shape[1]
    for slot in range(slots):
        for half, ref in enumerate((x_ref, dy_ref)):
            long_ref[slot, half * channels : (half + 1) * channels, :] = shifted_right(
                ref[slot].astype(jnp.float32)
            ).astype(jnp.bfloat16)
    long_ref[slots] = jnp.zeros(long_ref.shape[1:], jnp.bfloat16)
    width = one_ref.shape[1]
    third = width // 3
    both = jnp.concatenate(
        [one_ref[...].astype(jnp.float32), two_ref[...].astype(jnp.float32)], axis=0
    )
    for p in range(3):
        part = both[:, p * third : (p + 1) * third].astype(jnp.bfloat16)
        one_straight[p * channels : (p + 1) * channels, :] = part[:channels]
        two_straight[p * channels : (p + 1) * channels, :] = part[channels:]
    taps = width // channels
    spare = -width % LANES
    flipped = jnp.concatenate([both, jnp.zeros((2 * channels, spare), jnp.float32)], axis=1).T
    front = lax.broadcasted_iota(jnp.int32, (channels, LANES), 1) < PLANE

    def block(tap):
        return flipped[tap * channels : (tap + 1) * channels, :]

    for p in range(3):
        band = slice(p * channels, (p + 1) * channels)
        for start in range(0, 9, 2):
            here = block(taps - 1 - (9 * p + start))
            lanes = slice(start * channels, min(start + 2, 9) * channels)
            if start + 1 < 9:
                after = block(taps - 1 - (9 * p + start + 1))
                one = jnp.where(front, here, pltpu.roll(after, PLANE, 1))
                two = jnp.where(front, pltpu.roll(here, PLANE, 1), after)
            else:
                one, two = here[:, :channels], pltpu.roll(here, PLANE, 1)[:, :channels]
            one_turned[band, lanes] = one.astype(jnp.bfloat16)
            two_turned[band, lanes] = two.astype(jnp.bfloat16)


def gather_sides(slots, low_ref, high_ref, low, high):
    for slot in range(slots):
        low[slot] = low_ref[slot]
        high[slot] = high_ref[slot]
    low[slots] = jnp.zeros(low.shape[1:], jnp.bfloat16)
    high[slots] = jnp.zeros(high.shape[1:], jnp.bfloat16)


def spread(j, slots, link, long_ref, low, high, edge_ref, move_ref, mixed, outs):
    rows = long_ref.shape[1]
    channels = rows // 2
    place = {}
    for p in SIDES:
        for q, r in RING:
            if (p, q, r) == (0, 0, 0):
                place[p, q, r] = j
                continue
            number = 9 * (p + 1) + 3 * (q + 1) + (r + 1)
            number = number if number < 13 else number - 1
            found = link[j, 0, number]
            place[p, q, r] = jnp.where(found < 0, slots, found)
    one = jnp.ones((16, LANES), jnp.bfloat16)
    for tile in range(LONG // LANES):
        span = slice(tile * LANES, (tile + 1) * LANES)
        edge = {
            name: edge_ref[k, :, span]
            for k, name in enumerate((("q", -1), ("q", 1), ("r", -1), ("r", 1)))
        }
        inner = {name: one - value for name, value in edge.items()}
        for part in range(rows // 16):
            band = slice(part * 16, (part + 1) * 16)
            raw = {}
            for q, r in RING:
                value = long_ref[place[0, q, r], band, span]
                if tile == 0:
                    value = value + low[place[-1, q, r], band, :]
                if tile == LONG // LANES - 1:
                    value = value + high[place[1, q, r], band, :]
                raw[q, r] = value
            for r in (-1, 1):
                for q in SIDES:
                    raw[q, r] = raw[q, 0] * inner["r", r] + raw[q, r] * edge["r", r]
            for number, (q, r) in enumerate(TURNS):
                value = raw[q, r]
                if q != 0:
                    value = raw[0, r] * inner["q", q] + raw[q, r] * edge["q", q]
                mixed[number, band, span] = value
            half, start = divmod(part * 16, channels)
            start += 4 * channels
            outs[half][start : start + 16, span] = raw[0, 0]
    for number, (q, r) in enumerate(TURNS):
        start = RING.index((q, r)) * channels
        for low_lane in range(0, LONG, 4 * PLANE):
            width = min(4 * PLANE, LONG - low_lane)
            moved = jnp.dot(
                mixed[number, :, low_lane : low_lane + width],
                move_ref[number, :width, :width],
                preferred_element_type=jnp.float32,
            ).astype(jnp.bfloat16)
            for half in range(2):
                outs[half][start : start + channels, low_lane : low_lane + width] = moved[
                    half * channels : (half + 1) * channels
                ]


def convolved(weight_ref, field):
    channels = weight_ref.shape[0] // 3
    parts = jnp.dot(weight_ref[...], field[...], preferred_element_type=jnp.float32)
    middle = pltpu.roll(parts[channels : 2 * channels], LONG - PLANE, 1)
    return (
        parts[:channels, :CELLS] + middle[:, :CELLS] + parts[2 * channels :, LONG - CELLS :]
    )


def three_ways(values, moved):
    tail = jnp.zeros((values.shape[0], LONG - CELLS), jnp.float32)
    return jnp.concatenate(
        [
            jnp.concatenate([values, tail], axis=1).astype(jnp.bfloat16),
            moved,
            jnp.concatenate([tail, values], axis=1).astype(jnp.bfloat16),
        ],
        axis=0,
    )


def first_half(
    link, count, long_ref, low_ref, high_ref, edge_ref, move_ref, one_ref, two_ref,
    inner_ref, last_ref, first_ref, keep_ref, give_ref,
    low, high, mixed, field_x, field_dy, sum_one, sum_two, *, levels,
):
    slots = low_ref.shape[0]
    channels = long_ref.shape[1] // 2
    gather_sides(slots, low_ref, high_ref, low, high)
    sum_one[...] = jnp.zeros_like(sum_one)
    sum_two[...] = jnp.zeros_like(sum_two)
    inner_ref[...] = jnp.zeros_like(inner_ref)

    def visit(j, carry):
        spread(
            j, slots, link, long_ref, low, high, edge_ref, move_ref, mixed, (field_x, field_dy)
        )
        pre = convolved(one_ref, field_x)
        grad_hidden = convolved(two_ref, field_dy)
        sigma = 1.0 / (1.0 + jnp.exp(-pre))
        hidden = pre * sigma
        grad_pre = grad_hidden * (sigma * (1.0 + pre * (1.0 - sigma)))
        hidden_long = shifted_right(hidden).astype(jnp.bfloat16)
        grad_long = shifted_right(grad_pre).astype(jnp.bfloat16)
        inner_ref[j, :channels, :] = hidden_long
        inner_ref[j, channels:, :] = grad_long
        sum_one[...] += lax.dot_general(
            three_ways(grad_pre, grad_long),
            field_x[...],
            (((1,), (1,)), ((), ())),
            preferred_element_type=jnp.float32,
        )
        sum_two[...] += lax.dot_general(
            field_dy[...],
            three_ways(hidden, hidden_long),
            (((1,), (1,)), ((), ())),
            preferred_element_type=jnp.float32,
        )
        return carry

    lax.fori_loop(0, count[0, 0], visit, 0)
    for slot in range(slots):
        last_ref[slot] = inner_ref[slot, :, LONG - LANES :]
        first_ref[slot] = inner_ref[slot, :, :LANES]
    halves = [keep_ref, give_ref]
    upper = spot(levels[:1]) == 1

    def write(one_ref, two_ref):
        one_ref[...] = jnp.concatenate(
            [sum_one[p * channels : (p + 1) * channels, :] for p in range(3)], axis=1
        )
        blocks = []
        for tap in range(27):
            p, rest = divmod(26 - tap, 9)
            blocks.append(
                sum_two[rest * channels : (rest + 1) * channels, p * channels : (p + 1) * channels]
            )
        two_ref[...] = jnp.concatenate(blocks, axis=1)

    @pl.when(jnp.logical_not(upper))
    def _():
        write(*halves)

    @pl.when(upper)
    def _():
        write(*halves[::-1])


def spot(levels):
    place = 0
    for k, (axis, reach) in enumerate(levels):
        place = place + (lax.axis_index(axis) // reach) % 2 * 2**k
    return place


def scatter(keep_ref, got_ref, *refs, levels):
    *outs, total_ref = refs
    total_ref[...] = keep_ref[...] + got_ref[...]
    rows = outs[0].shape[0]
    mine = spot(levels)
    for k, out in enumerate(outs):
        start = pl.multiple_of((mine ^ k) * rows, 16)
        out[...] = total_ref[pl.ds(start, rows), :].astype(out.dtype)


def paired_sum(*refs):
    *parts, out_ref = refs
    parts = [part[...].astype(jnp.float32) for part in parts]
    while len(parts) > 1:
        parts = [first + second for first, second in zip(parts[::2], parts[1::2])]
    out_ref[...] = parts[0].astype(out_ref.dtype)


def gather(*refs, levels):
    *parts, out_ref = refs
    rows = parts[0].shape[0]
    mine = spot(levels)
    for k, part in enumerate(parts):
        out_ref[pl.ds(pl.multiple_of((mine ^ k) * rows, 16), rows), :] = part[...]


def join_last(mine_ref, other_ref, one_ref, two_ref, *, levels, scale):
    upper = spot(levels) == 1
    mine = mine_ref[...].astype(jnp.float32) * scale
    other = other_ref[...].astype(jnp.float32) * scale
    one_ref[...] = jnp.where(upper, other, mine)
    two_ref[...] = jnp.where(upper, mine, other)


def place(count, *refs):
    out_ref = refs[-1]
    arrived = refs[1][...]
    for ref in refs[2:-1]:
        arrived = arrived + ref[...]
    for slot in range(out_ref.shape[0]):
        out_ref[slot] = jnp.where(count[0, 0] == slot, arrived, refs[0][slot])


def second_half(begin, end, refs, scratch, out_ref, back_ref):
    link, count, inner_ref, low_ref, high_ref, edge_ref, move_ref, two_ref, one_ref, x_ref, dy_ref = (
        refs
    )
    low, high, mixed, field_h, field_g = scratch
    slots = low_ref.shape[0]
    gather_sides(slots, low_ref, high_ref, low, high)

    def visit(j, carry):
        spread(
            j, slots, link, inner_ref, low, high, edge_ref, move_ref, mixed, (field_h, field_g)
        )
        out = convolved(two_ref, field_h)
        back = convolved(one_ref, field_g).astype(jnp.bfloat16)
        out_ref[j - begin] = (x_ref[j].astype(jnp.float32) + out).astype(jnp.bfloat16)
        back_ref[j - begin] = (dy_ref[j].astype(jnp.float32) + back.astype(jnp.float32)).astype(
            jnp.bfloat16
        )
        return carry

    lax.fori_loop(begin, jnp.minimum(count[0, 0], end), visit, 0)


def second_surplus(*refs):
    slots = refs[3].shape[0]
    inputs, back_ref, (*moved, out), scratch = refs[:11], refs[11], refs[12:-5], refs[-5:]
    out[...] = jnp.zeros_like(out)
    back_ref[...] = jnp.zeros_like(back_ref)
    second_half(WORK_CAP, slots, inputs, scratch, out, back_ref)
    for number, ref in enumerate(moved):
        ref[...] = out[number]


def second_own(*refs):
    inputs, (part_ref, own_ref, back_ref), scratch = refs[:11], refs[11:14], refs[14:]
    own_ref[...] = jnp.zeros_like(own_ref)
    back_ref[:WORK_CAP] = jnp.zeros_like(own_ref)
    back_ref[WORK_CAP:] = part_ref[...]
    second_half(0, WORK_CAP, inputs, scratch, own_ref, back_ref)


def vmem(count):
    return [pl.BlockSpec(memory_space=pltpu.VMEM)] * count


def smem(count):
    return [pl.BlockSpec(memory_space=pltpu.SMEM)] * count


def step_to(x, by, wrap):
    size = lax.axis_size("space")
    pairs = [(i, (i + by) % size) for i in range(size) if wrap or 0 <= i + by < size]
    return lax.ppermute(x, "space", pairs)


def groups_of():
    levels = [
        (axis, 2**k)
        for axis in ("space", "batch")
        for k in range(int(math.log2(lax.axis_size(axis))))
    ]
    rest = levels[2:-1]
    pairs = [tuple(rest[k : k + 2]) for k in range(0, len(rest), 2)]
    return [(levels[0],), (levels[1], levels[-1])] + pairs


def all_sum(keep, give, groups, scale):
    shape = jax.ShapeDtypeStruct
    params = pltpu.CompilerParams(vmem_limit_bytes=6 * 2**20)
    bf16 = jnp.bfloat16

    def swap(value, levels, number):
        reach = {"batch": 0, "space": 0}
        for k, (axis, by) in enumerate(levels):
            reach[axis] += by * (number >> k & 1)
        width = lax.axis_size("space")
        pairs = [
            (i, ((i // width ^ reach["batch"]) * width) + (i % width ^ reach["space"]))
            for i in range(lax.axis_size("batch") * width)
        ]
        return lax.ppermute(value, ("batch", "space"), pairs)

    def call(body, outs, *arrays, scratch=(), **static):
        outs = [shape(*out) for out in outs]
        return pl.pallas_call(
            partial(body, **static),
            out_shape=outs,
            in_specs=vmem(len(arrays)),
            out_specs=vmem(len(outs)),
            scratch_shapes=scratch,
            compiler_params=params,
        )(*arrays)

    width = keep.shape[1]
    whole = (keep.shape, jnp.float32)
    pair, spread_over, *others = groups
    got = swap(give, pair, 1)
    members = 2 ** len(spread_over)
    part = (keep.shape[0] // members, width)
    mine, *gives = call(
        scatter,
        [(part, jnp.float32)] + [(part, bf16)] * (members - 1),
        keep,
        got,
        levels=spread_over,
        scratch=[pltpu.VMEM(keep.shape, jnp.float32)],
    )
    gots = [swap(value, spread_over, k + 1) for k, value in enumerate(gives)]
    (mine,) = call(paired_sum, [(part, bf16)], mine, *gots)
    for group in others:
        gots = [swap(mine, group, k) for k in range(1, 2 ** len(group))]
        (mine,) = call(paired_sum, [(part, bf16)], mine, *gots)
    gots = [swap(mine, spread_over, k) for k in range(1, members)]
    (mine,) = call(gather, [(keep.shape, bf16)], mine, *gots, levels=spread_over)
    other = swap(mine, pair, 1)
    return call(join_last, [whole, whole], mine, other, levels=pair, scale=scale)


def shards(features, cotangent, brick_count, destination, neighbours, kernel_one, kernel_two):
    slots, channels = features.shape[1], features.shape[2]
    x, dy = features[0], cotangent[0]
    count = brick_count
    link = neighbours.transpose(2, 0, 1)
    bf16, f32 = jnp.bfloat16, jnp.float32
    shape = jax.ShapeDtypeStruct
    long_shape = shape((slots + 1, 2 * channels, LONG), bf16)
    side_shape = shape((slots, 2 * channels, LANES), bf16)
    moves, edges = turn_tables()
    params = pltpu.CompilerParams(vmem_limit_bytes=20 * 2**20)

    far = pl.BlockSpec(memory_space=pltpu.HBM)
    last, first = pl.pallas_call(
        sides,
        out_shape=(side_shape, side_shape),
        in_specs=[far, far],
        out_specs=tuple(vmem(2)),
        scratch_shapes=[
            pltpu.VMEM((2, slots, channels, LANES), bf16),
            pltpu.VMEM((2, slots, channels, LANES), bf16),
            pltpu.SemaphoreType.DMA((2, 2)),
        ],
        compiler_params=params,
        name="sides",
    )(x, dy)
    weight_shape = shape((3 * channels, 9 * channels), bf16)
    long_in, one_straight, two_straight, one_turned, two_turned = pl.pallas_call(
        prepare,
        out_shape=(long_shape,) + (weight_shape,) * 4,
        in_specs=[far] * 4,
        out_specs=tuple(vmem(5)),
        scratch_shapes=[
            pltpu.VMEM(x.shape, bf16),
            pltpu.VMEM(x.shape, bf16),
            pltpu.VMEM(kernel_one.shape, bf16),
            pltpu.VMEM(kernel_one.shape, bf16),
            pltpu.SemaphoreType.DMA((4,)),
        ],
        compiler_params=params,
        name="prepare",
    )(x, dy, kernel_one, kernel_two)
    low = step_to(last, 1, False)
    high = step_to(first, -1, False)
    side_scratch = pltpu.VMEM((slots + 1, 2 * channels, LANES), bf16)
    mixed_scratch = pltpu.VMEM((len(TURNS), 2 * channels, LONG), bf16)
    field_scratch = pltpu.VMEM((9 * channels, LONG), bf16)
    groups = groups_of()
    half_shape = shape(kernel_one.shape, f32)
    inner, inner_last, inner_first, keep, give = pl.pallas_call(
        partial(first_half, levels=groups[0]),
        out_shape=(
            long_shape,
            side_shape,
            side_shape,
            half_shape,
            half_shape,
        ),
        in_specs=smem(2) + vmem(7),
        out_specs=tuple(vmem(5)),
        scratch_shapes=[
            side_scratch,
            side_scratch,
            mixed_scratch,
            field_scratch,
            field_scratch,
            pltpu.VMEM((3 * channels, 9 * channels), f32),
            pltpu.VMEM((9 * channels, 3 * channels), f32),
        ],
        compiler_params=params,
        name="first_half",
    )(link, count, long_in, low, high, edges, moves, one_straight, two_turned)
    inner_low = step_to(inner_last, 1, False)
    inner_high = step_to(inner_first, -1, False)
    surplus = slots - WORK_CAP
    brick = shape(x.shape[1:], bf16)
    inputs = (
        link, count, inner, inner_low, inner_high, edges, moves, two_straight, one_turned, x, dy
    )
    scratch = [side_scratch, side_scratch, mixed_scratch, field_scratch, field_scratch]
    surplus_shape = (surplus,) + x.shape[1:]
    part, *moved = pl.pallas_call(
        second_surplus,
        out_shape=(shape(surplus_shape, bf16),) + (brick,) * surplus,
        in_specs=smem(2) + vmem(9),
        out_specs=tuple(vmem(1 + surplus)),
        scratch_shapes=[pltpu.VMEM(surplus_shape, bf16)] + scratch,
        compiler_params=params,
        name="second_surplus",
    )(*inputs)
    own, grad_in = pl.pallas_call(
        second_own,
        out_shape=(shape((WORK_CAP,) + x.shape[1:], bf16), shape(x.shape, bf16)),
        in_specs=smem(2) + vmem(10),
        out_specs=tuple(vmem(2)),
        scratch_shapes=scratch,
        compiler_params=params,
        name="second_own",
    )(*inputs, part)
    arrived = []
    for number, brick_out in enumerate(moved):
        arrived.append(step_to(brick_out, number + 1, True))
    placed = pl.pallas_call(
        place,
        out_shape=shape(own.shape, bf16),
        in_specs=smem(1) + vmem(1 + surplus),
        out_specs=pl.BlockSpec(memory_space=pltpu.VMEM),
        compiler_params=params,
        name="place",
    )(count, own, *arrived)
    scale = 1.0 / math.sqrt(
        lax.axis_size("batch") * features.shape[0] * lax.axis_size("space") * slots * CELLS
    )
    grad_one, grad_two = all_sum(keep, give, groups, scale)
    return (placed[None], grad_in[None], grad_one, grad_two)


def solution(mesh):
    return whole_step(mesh, shards)


def whole_step(mesh, step):
    return jax.shard_map(
        step,
        mesh=mesh,
        in_specs=(
            P("batch", "space", None, None),
            P("batch", "space", None, None),
            P("batch", "space"),
            P("batch", "space"),
            P("batch", None, "space"),
            P(),
            P(),
        ),
        out_specs=(P("batch", "space", None, None), P("batch", "space", None, None), P(), P()),
        check_vma=False,
    )
```

```python
import math
from functools import partial

import jax
import jax.numpy as jnp
import numpy as np
from jax import lax
from jax.experimental import pallas as pl
from jax.experimental.pallas import tpu as pltpu
from jax.sharding import PartitionSpec as P


EDGE = 8
WORK_CAP = 2
CELLS = EDGE**3
PLANE = EDGE * EDGE
LONG = CELLS + 2 * PLANE
LANES = 128
SIDES = (-1, 0, 1)
RING = [(q, r) for q in SIDES for r in SIDES]
TURNS = [(q, r) for q, r in RING if (q, r) != (0, 0)]


def edge_table():
    lane = np.arange(LONG) % PLANE
    edges = np.stack(
        [
            lane // EDGE == EDGE - 1,
            lane // EDGE == 0,
            lane % EDGE == EDGE - 1,
            lane % EDGE == 0,
        ]
    ).astype(np.float32)
    return jnp.asarray(np.broadcast_to(edges[:, None, :], (4, 16, LONG)), jnp.bfloat16)


def shifted_right(values):
    tail = jnp.zeros((values.shape[0], LONG - CELLS), jnp.float32)
    return pltpu.roll(jnp.concatenate([values, tail], axis=1), PLANE, 1)


def sides(x_ref, dy_ref, last_ref, first_ref, begin, end, sems):
    slots, channels = x_ref.shape[0], x_ref.shape[1]
    copies = []
    for half, ref in enumerate((x_ref, dy_ref)):
        for number, (box, at) in enumerate(((begin, 0), (end, CELLS - LANES))):
            copies.append(
                pltpu.make_async_copy(
                    ref.at[:, :, pl.ds(at, LANES)], box.at[half], sems.at[half, number]
                )
            )
    for copy in copies:
        copy.start()
    for copy in copies:
        copy.wait()
    front = lax.broadcasted_iota(jnp.int32, (channels, LANES), 1) < PLANE
    for slot in range(slots):
        late, late_dy = (end[half, slot].astype(jnp.float32) for half in range(2))
        late = jnp.where(front, pltpu.roll(late, PLANE, 1), late_dy)
        last_ref[slot] = late.astype(jnp.bfloat16)
        early, early_dy = (begin[half, slot].astype(jnp.float32) for half in range(2))
        early = jnp.where(front, early_dy, pltpu.roll(early, PLANE, 1))
        first_ref[slot] = early.astype(jnp.bfloat16)


def prepare(
    link, x_far, dy_far, one_far, two_far,
    link_ref, long_ref, one_straight, two_straight, one_turned, two_turned, move_ref,
    x_ref, dy_ref, one_ref, two_ref, sems,
):
    pairs = ((x_far, x_ref), (dy_far, dy_ref), (one_far, one_ref), (two_far, two_ref))
    copies = [
        pltpu.make_async_copy(far, near, sems.at[k]) for k, (far, near) in enumerate(pairs)
    ]
    for copy in copies:
        copy.start()
    for slot in range(link.shape[0]):
        for number in range(link.shape[2]):
            link_ref[slot, 0, number] = link[slot, 0, number]
    size = move_ref.shape[1]
    lane = lax.broadcasted_iota(jnp.int32, (EDGE, size), 1)
    origin = lax.broadcasted_iota(jnp.int32, (size, size), 0)
    for number, (q, r) in enumerate(TURNS):
        row = (lane // EDGE + q) & (EDGE - 1)
        column = (lane + r) & (EDGE - 1)
        source = (lane & -PLANE) + row * EDGE + column
        source = jnp.broadcast_to(source[:1], (size, size))
        move_ref[number] = jnp.where(origin == source, 1.0, 0.0).astype(jnp.bfloat16)
    for copy in copies:
        copy.wait()
    slots, channels = x_ref.shape[0], x_ref.shape[1]
    for slot in range(slots):
        for half, ref in enumerate((x_ref, dy_ref)):
            long_ref[slot, half * channels : (half + 1) * channels, :] = shifted_right(
                ref[slot].astype(jnp.float32)
            ).astype(jnp.bfloat16)
    long_ref[slots] = jnp.zeros(long_ref.shape[1:], jnp.bfloat16)
    width = one_ref.shape[1]
    third = width // 3
    both = jnp.concatenate(
        [one_ref[...].astype(jnp.float32), two_ref[...].astype(jnp.float32)], axis=0
    )
    for p in range(3):
        part = both[:, p * third : (p + 1) * third].astype(jnp.bfloat16)
        one_straight[p * channels : (p + 1) * channels, :] = part[:channels]
        two_straight[p * channels : (p + 1) * channels, :] = part[channels:]
    taps = width // channels
    spare = -width % LANES
    flipped = jnp.concatenate([both, jnp.zeros((2 * channels, spare), jnp.float32)], axis=1).T
    front = lax.broadcasted_iota(jnp.int32, (channels, LANES), 1) < PLANE

    def block(tap):
        return flipped[tap * channels : (tap + 1) * channels, :]

    for p in range(3):
        band = slice(p * channels, (p + 1) * channels)
        for start in range(0, 9, 2):
            here = block(taps - 1 - (9 * p + start))
            lanes = slice(start * channels, min(start + 2, 9) * channels)
            if start + 1 < 9:
                after = block(taps - 1 - (9 * p + start + 1))
                one = jnp.where(front, here, pltpu.roll(after, PLANE, 1))
                two = jnp.where(front, pltpu.roll(here, PLANE, 1), after)
            else:
                one, two = here[:, :channels], pltpu.roll(here, PLANE, 1)[:, :channels]
            one_turned[band, lanes] = one.astype(jnp.bfloat16)
            two_turned[band, lanes] = two.astype(jnp.bfloat16)


def gather_sides(slots, low_ref, high_ref, low, high):
    channels = low_ref.shape[1]
    front = lax.broadcasted_iota(jnp.int32, (channels, LANES), 1) < PLANE
    for slot in range(slots):
        for half in range(2):
            band = slice(half * channels, (half + 1) * channels)
            below = low_ref[slot].astype(jnp.float32)
            above = high_ref[slot].astype(jnp.float32)
            if half:
                below, above = pltpu.roll(below, PLANE, 1), pltpu.roll(above, PLANE, 1)
            low[slot, band, :] = jnp.where(front, below, 0.0).astype(jnp.bfloat16)
            high[slot, band, :] = jnp.where(front, 0.0, above).astype(jnp.bfloat16)
    low[slots] = jnp.zeros(low.shape[1:], jnp.bfloat16)
    high[slots] = jnp.zeros(high.shape[1:], jnp.bfloat16)


def spread(j, slots, link, long_ref, low, high, edge_ref, move_ref, mixed, outs):
    rows = long_ref.shape[1]
    channels = rows // 2
    place = {}
    for p in SIDES:
        for q, r in RING:
            if (p, q, r) == (0, 0, 0):
                place[p, q, r] = j
                continue
            number = 9 * (p + 1) + 3 * (q + 1) + (r + 1)
            number = number if number < 13 else number - 1
            found = link[j, 0, number]
            place[p, q, r] = jnp.where(found < 0, slots, found)
    one = jnp.ones((16, LANES), jnp.bfloat16)
    for tile in range(LONG // LANES):
        span = slice(tile * LANES, (tile + 1) * LANES)
        edge = {
            name: edge_ref[k, :, span]
            for k, name in enumerate((("q", -1), ("q", 1), ("r", -1), ("r", 1)))
        }
        inner = {name: one - value for name, value in edge.items()}
        for part in range(rows // 16):
            band = slice(part * 16, (part + 1) * 16)
            raw = {}
            for q, r in RING:
                value = long_ref[place[0, q, r], band, span]
                if tile == 0:
                    value = value + low[place[-1, q, r], band, :]
                if tile == LONG // LANES - 1:
                    value = value + high[place[1, q, r], band, :]
                raw[q, r] = value
            for r in (-1, 1):
                for q in SIDES:
                    raw[q, r] = raw[q, 0] * inner["r", r] + raw[q, r] * edge["r", r]
            for number, (q, r) in enumerate(TURNS):
                value = raw[q, r]
                if q != 0:
                    value = raw[0, r] * inner["q", q] + raw[q, r] * edge["q", q]
                mixed[number, band, span] = value
            half, start = divmod(part * 16, channels)
            start += 4 * channels
            outs[half][start : start + 16, span] = raw[0, 0]
    for number, (q, r) in enumerate(TURNS):
        start = RING.index((q, r)) * channels
        for low_lane in range(0, LONG, 4 * PLANE):
            width = min(4 * PLANE, LONG - low_lane)
            moved = jnp.dot(
                mixed[number, :, low_lane : low_lane + width],
                move_ref[number, :width, :width],
                preferred_element_type=jnp.float32,
            ).astype(jnp.bfloat16)
            for half in range(2):
                outs[half][start : start + channels, low_lane : low_lane + width] = moved[
                    half * channels : (half + 1) * channels
                ]


def convolved(weight_ref, field):
    channels = weight_ref.shape[0] // 3
    parts = jnp.dot(weight_ref[...], field[...], preferred_element_type=jnp.float32)
    middle = pltpu.roll(parts[channels : 2 * channels], LONG - PLANE, 1)
    return (
        parts[:channels, :CELLS] + middle[:, :CELLS] + parts[2 * channels :, LONG - CELLS :]
    )


def three_ways(values, moved):
    tail = jnp.zeros((values.shape[0], LONG - CELLS), jnp.float32)
    return jnp.concatenate(
        [
            jnp.concatenate([values, tail], axis=1).astype(jnp.bfloat16),
            moved,
            jnp.concatenate([tail, values], axis=1).astype(jnp.bfloat16),
        ],
        axis=0,
    )


def first_half(
    link, count, long_ref, low_ref, high_ref, edge_ref, move_ref, one_ref, two_ref,
    inner_ref, last_ref, first_ref, keep_ref, give_ref,
    low, high, mixed, field_x, field_dy, sum_one, sum_two, *, levels,
):
    slots = low_ref.shape[0]
    channels = long_ref.shape[1] // 2
    gather_sides(slots, low_ref, high_ref, low, high)
    sum_one[...] = jnp.zeros_like(sum_one)
    sum_two[...] = jnp.zeros_like(sum_two)
    inner_ref[...] = jnp.zeros_like(inner_ref)

    def visit(j, carry):
        spread(
            j, slots, link, long_ref, low, high, edge_ref, move_ref, mixed, (field_x, field_dy)
        )
        pre = convolved(one_ref, field_x)
        grad_hidden = convolved(two_ref, field_dy)
        sigma = 1.0 / (1.0 + jnp.exp(-pre))
        hidden = pre * sigma
        grad_pre = grad_hidden * (sigma * (1.0 + pre * (1.0 - sigma)))
        hidden_long = shifted_right(hidden).astype(jnp.bfloat16)
        grad_long = shifted_right(grad_pre).astype(jnp.bfloat16)
        inner_ref[j, :channels, :] = hidden_long
        inner_ref[j, channels:, :] = grad_long
        sum_one[...] += lax.dot_general(
            three_ways(grad_pre, grad_long),
            field_x[...],
            (((1,), (1,)), ((), ())),
            preferred_element_type=jnp.float32,
        )
        sum_two[...] += lax.dot_general(
            field_dy[...],
            three_ways(hidden, hidden_long),
            (((1,), (1,)), ((), ())),
            preferred_element_type=jnp.float32,
        )
        return carry

    lax.fori_loop(0, count[0, 0], visit, 0)
    for slot in range(slots):
        for ref, start in ((last_ref, LONG - LANES), (first_ref, 0)):
            plane = inner_ref[slot, :, start : start + LANES].astype(jnp.float32)
            plane = plane[:channels] + pltpu.roll(plane[channels:], PLANE, 1)
            ref[slot] = plane.astype(jnp.bfloat16)
    halves = [keep_ref, give_ref]
    upper = spot(levels[:1]) == 1

    def write(one_ref, two_ref):
        one_ref[...] = jnp.concatenate(
            [sum_one[p * channels : (p + 1) * channels, :] for p in range(3)], axis=1
        )
        blocks = []
        for tap in range(27):
            p, rest = divmod(26 - tap, 9)
            blocks.append(
                sum_two[rest * channels : (rest + 1) * channels, p * channels : (p + 1) * channels]
            )
        two_ref[...] = jnp.concatenate(blocks, axis=1)

    @pl.when(jnp.logical_not(upper))
    def _():
        write(*halves)

    @pl.when(upper)
    def _():
        write(*halves[::-1])


def spot(levels):
    place = 0
    for k, (axis, reach) in enumerate(levels):
        place = place + (lax.axis_index(axis) // reach) % 2 * 2**k
    return place


def scatter(keep_ref, got_ref, *refs, levels):
    *outs, total_ref = refs
    total_ref[...] = keep_ref[...] + got_ref[...]
    rows = outs[0].shape[0]
    mine = spot(levels)
    for k, out in enumerate(outs):
        start = pl.multiple_of((mine ^ k) * rows, 16)
        out[...] = total_ref[pl.ds(start, rows), :].astype(out.dtype)


def paired_sum(*refs):
    *parts, out_ref = refs
    parts = [part[...].astype(jnp.float32) for part in parts]
    while len(parts) > 1:
        parts = [first + second for first, second in zip(parts[::2], parts[1::2])]
    out_ref[...] = parts[0].astype(out_ref.dtype)


def gather(*refs, levels):
    *parts, out_ref = refs
    rows = parts[0].shape[0]
    mine = spot(levels)
    for k, part in enumerate(parts):
        out_ref[pl.ds(pl.multiple_of((mine ^ k) * rows, 16), rows), :] = part[...]


def join_last(mine_ref, other_ref, one_ref, two_ref, *, levels, scale):
    upper = spot(levels) == 1
    mine = mine_ref[...].astype(jnp.float32) * scale
    other = other_ref[...].astype(jnp.float32) * scale
    one_ref[...] = jnp.where(upper, other, mine)
    two_ref[...] = jnp.where(upper, mine, other)


def place(count, *refs):
    out_ref = refs[-1]
    arrived = refs[1][...]
    for ref in refs[2:-1]:
        arrived = arrived + ref[...]
    for slot in range(out_ref.shape[0]):
        out_ref[slot] = jnp.where(count[0, 0] == slot, arrived, refs[0][slot])


def second_half(begin, end, refs, scratch, out_ref, back_ref):
    link, count, inner_ref, low_ref, high_ref, edge_ref, move_ref, two_ref, one_ref, x_ref, dy_ref = (
        refs
    )
    low, high, mixed, field_h, field_g = scratch
    slots = low_ref.shape[0]
    gather_sides(slots, low_ref, high_ref, low, high)

    def visit(j, carry):
        spread(
            j, slots, link, inner_ref, low, high, edge_ref, move_ref, mixed, (field_h, field_g)
        )
        out = convolved(two_ref, field_h)
        back = convolved(one_ref, field_g).astype(jnp.bfloat16)
        out_ref[j - begin] = (x_ref[j].astype(jnp.float32) + out).astype(jnp.bfloat16)
        back_ref[j - begin] = (dy_ref[j].astype(jnp.float32) + back.astype(jnp.float32)).astype(
            jnp.bfloat16
        )
        return carry

    lax.fori_loop(begin, jnp.minimum(count[0, 0], end), visit, 0)


def second_surplus(*refs):
    slots = refs[3].shape[0]
    inputs, back_ref, (*moved, out), scratch = refs[:11], refs[11], refs[12:-5], refs[-5:]
    out[...] = jnp.zeros_like(out)
    back_ref[...] = jnp.zeros_like(back_ref)
    second_half(WORK_CAP, slots, inputs, scratch, out, back_ref)
    for number, ref in enumerate(moved):
        ref[...] = out[number]


def second_own(*refs):
    inputs, (part_ref, own_ref, back_ref), scratch = refs[:11], refs[11:14], refs[14:]
    own_ref[...] = jnp.zeros_like(own_ref)
    back_ref[:WORK_CAP] = jnp.zeros_like(own_ref)
    back_ref[WORK_CAP:] = part_ref[...]
    second_half(0, WORK_CAP, inputs, scratch, own_ref, back_ref)


def vmem(count):
    return [pl.BlockSpec(memory_space=pltpu.VMEM)] * count


def smem(count):
    return [pl.BlockSpec(memory_space=pltpu.SMEM)] * count


def step_to(x, by, wrap):
    size = lax.axis_size("space")
    pairs = [(i, (i + by) % size) for i in range(size) if wrap or 0 <= i + by < size]
    return lax.ppermute(x, "space", pairs)


def groups_of():
    levels = [
        (axis, 2**k)
        for axis in ("space", "batch")
        for k in range(int(math.log2(lax.axis_size(axis))))
    ]
    rest = levels[2:-1]
    pairs = [tuple(rest[k : k + 2]) for k in range(0, len(rest), 2)]
    return [(levels[0],), (levels[1], levels[-1])] + pairs


def all_sum(keep, give, groups, scale):
    shape = jax.ShapeDtypeStruct
    params = pltpu.CompilerParams(vmem_limit_bytes=6 * 2**20)
    bf16 = jnp.bfloat16

    def swap(value, levels, number):
        reach = {"batch": 0, "space": 0}
        for k, (axis, by) in enumerate(levels):
            reach[axis] += by * (number >> k & 1)
        width = lax.axis_size("space")
        pairs = [
            (i, ((i // width ^ reach["batch"]) * width) + (i % width ^ reach["space"]))
            for i in range(lax.axis_size("batch") * width)
        ]
        return lax.ppermute(value, ("batch", "space"), pairs)

    def call(body, outs, *arrays, scratch=(), **static):
        outs = [shape(*out) for out in outs]
        return pl.pallas_call(
            partial(body, **static),
            out_shape=outs,
            in_specs=vmem(len(arrays)),
            out_specs=vmem(len(outs)),
            scratch_shapes=scratch,
            compiler_params=params,
        )(*arrays)

    width = keep.shape[1]
    whole = (keep.shape, jnp.float32)
    pair, spread_over, *others = groups
    got = swap(give, pair, 1)
    members = 2 ** len(spread_over)
    part = (keep.shape[0] // members, width)
    mine, *gives = call(
        scatter,
        [(part, jnp.float32)] + [(part, bf16)] * (members - 1),
        keep,
        got,
        levels=spread_over,
        scratch=[pltpu.VMEM(keep.shape, jnp.float32)],
    )
    gots = [swap(value, spread_over, k + 1) for k, value in enumerate(gives)]
    (mine,) = call(paired_sum, [(part, bf16)], mine, *gots)
    for group in others:
        gots = [swap(mine, group, k) for k in range(1, 2 ** len(group))]
        (mine,) = call(paired_sum, [(part, bf16)], mine, *gots)
    gots = [swap(mine, spread_over, k) for k in range(1, members)]
    (mine,) = call(gather, [(keep.shape, bf16)], mine, *gots, levels=spread_over)
    other = swap(mine, pair, 1)
    return call(join_last, [whole, whole], mine, other, levels=pair, scale=scale)


def shards(features, cotangent, brick_count, destination, neighbours, kernel_one, kernel_two):
    slots, channels = features.shape[1], features.shape[2]
    x, dy = features[0], cotangent[0]
    count = brick_count
    link = neighbours.transpose(2, 0, 1)
    bf16, f32 = jnp.bfloat16, jnp.float32
    shape = jax.ShapeDtypeStruct
    long_shape = shape((slots + 1, 2 * channels, LONG), bf16)
    side_shape = shape((slots, channels, LANES), bf16)
    edges = edge_table()
    params = pltpu.CompilerParams(vmem_limit_bytes=20 * 2**20)

    far = pl.BlockSpec(memory_space=pltpu.HBM)
    last, first = pl.pallas_call(
        sides,
        out_shape=(side_shape, side_shape),
        in_specs=[far, far],
        out_specs=tuple(vmem(2)),
        scratch_shapes=[
            pltpu.VMEM((2, slots, channels, LANES), bf16),
            pltpu.VMEM((2, slots, channels, LANES), bf16),
            pltpu.SemaphoreType.DMA((2, 2)),
        ],
        compiler_params=params,
        name="sides",
    )(x, dy)
    weight_shape = shape((3 * channels, 9 * channels), bf16)
    link, long_in, one_straight, two_straight, one_turned, two_turned, moves = pl.pallas_call(
        prepare,
        out_shape=(shape(link.shape, link.dtype), long_shape)
        + (weight_shape,) * 4
        + (shape((len(TURNS), 4 * PLANE, 4 * PLANE), bf16),),
        in_specs=smem(1) + [far] * 4,
        out_specs=tuple(smem(1) + vmem(6)),
        scratch_shapes=[
            pltpu.VMEM(x.shape, bf16),
            pltpu.VMEM(x.shape, bf16),
            pltpu.VMEM(kernel_one.shape, bf16),
            pltpu.VMEM(kernel_one.shape, bf16),
            pltpu.SemaphoreType.DMA((4,)),
        ],
        compiler_params=params,
        name="prepare",
    )(link, x, dy, kernel_one, kernel_two)
    low = step_to(last, 1, False)
    high = step_to(first, -1, False)
    side_scratch = pltpu.VMEM((slots + 1, 2 * channels, LANES), bf16)
    mixed_scratch = pltpu.VMEM((len(TURNS), 2 * channels, LONG), bf16)
    field_scratch = pltpu.VMEM((9 * channels, LONG), bf16)
    groups = groups_of()
    half_shape = shape(kernel_one.shape, f32)
    inner, inner_last, inner_first, keep, give = pl.pallas_call(
        partial(first_half, levels=groups[0]),
        out_shape=(
            long_shape,
            side_shape,
            side_shape,
            half_shape,
            half_shape,
        ),
        in_specs=smem(2) + vmem(7),
        out_specs=tuple(vmem(5)),
        scratch_shapes=[
            side_scratch,
            side_scratch,
            mixed_scratch,
            field_scratch,
            field_scratch,
            pltpu.VMEM((3 * channels, 9 * channels), f32),
            pltpu.VMEM((9 * channels, 3 * channels), f32),
        ],
        compiler_params=params,
        name="first_half",
    )(link, count, long_in, low, high, edges, moves, one_straight, two_turned)
    inner_low = step_to(inner_last, 1, False)
    inner_high = step_to(inner_first, -1, False)
    surplus = slots - WORK_CAP
    brick = shape(x.shape[1:], bf16)
    inputs = (
        link, count, inner, inner_low, inner_high, edges, moves, two_straight, one_turned, x, dy
    )
    scratch = [side_scratch, side_scratch, mixed_scratch, field_scratch, field_scratch]
    surplus_shape = (surplus,) + x.shape[1:]
    part, *moved = pl.pallas_call(
        second_surplus,
        out_shape=(shape(surplus_shape, bf16),) + (brick,) * surplus,
        in_specs=smem(2) + vmem(9),
        out_specs=tuple(vmem(1 + surplus)),
        scratch_shapes=[pltpu.VMEM(surplus_shape, bf16)] + scratch,
        compiler_params=params,
        name="second_surplus",
    )(*inputs)
    own, grad_in = pl.pallas_call(
        second_own,
        out_shape=(shape((WORK_CAP,) + x.shape[1:], bf16), shape(x.shape, bf16)),
        in_specs=smem(2) + vmem(10),
        out_specs=tuple(vmem(2)),
        scratch_shapes=scratch,
        compiler_params=params,
        name="second_own",
    )(*inputs, part)
    arrived = []
    for number, brick_out in enumerate(moved):
        arrived.append(step_to(brick_out, number + 1, True))
    placed = pl.pallas_call(
        place,
        out_shape=shape(own.shape, bf16),
        in_specs=smem(1) + vmem(1 + surplus),
        out_specs=pl.BlockSpec(memory_space=pltpu.VMEM),
        compiler_params=params,
        name="place",
    )(count, own, *arrived)
    scale = 1.0 / math.sqrt(
        lax.axis_size("batch") * features.shape[0] * lax.axis_size("space") * slots * CELLS
    )
    grad_one, grad_two = all_sum(keep, give, groups, scale)
    return (placed[None], grad_in[None], grad_one, grad_two)


def solution(mesh):
    return whole_step(mesh, shards)


def whole_step(mesh, step):
    return jax.shard_map(
        step,
        mesh=mesh,
        in_specs=(
            P("batch", "space", None, None),
            P("batch", "space", None, None),
            P("batch", "space"),
            P("batch", "space"),
            P("batch", None, "space"),
            P(),
            P(),
        ),
        out_specs=(P("batch", "space", None, None), P("batch", "space", None, None), P(), P()),
        check_vma=False,
    )
```
